32 devices in a mesh: grp: 4 (over y, x), row: 8 (over z, core).
Axes of the slice: x: 2, y: 2, z: 4, core: 2. Of those that a mesh axis runs over, the one named last changes fastest.
Arguments:
- blocks: bfloat16 [32, 4, 10, 256, 256], P(('grp', 'row')), may hold values from 0 to 1
- columns: int32 [32, 4, 10], P(('grp', 'row')), may hold values from -1 to 31, as said below
- factor: bfloat16 [64, 8192], P(None, ('grp', 'row')), may hold values from 0 to 0.3, as said below
Outputs:
- updated: float32 [64, 8192], P(None, ('grp', 'row'))
The draws below stay inside these ranges and needn't reach their ends.
Inputs may be any that keep to these rules, and one draw needn't show every extreme that they name: Tile row i lies in group g = i // 8. In block h of tile row i the live slots come first and name distinct tile columns of group h (h * 8 to h * 8 + 7), none above i; block g always names i itself; blocks h > g are empty; a block holds at most 10 live slots, and -1 marks an empty slot. `factor`: entries are nonnegative.
All inputs are finite; a program needn't handle non-finite values.
Results may differ from the reference program's by a relative error of at most 0.0003.
Values may be sent and summed in bfloat16 or wider, within the bound.
No kernel may reach another device: no remote copies, remote signals or barrier semaphores. Data moves between devices by JAX's collectives and lax.ppermute only.
A program may use at most 128 MiB of HBM per device.

```python
import jax
import jax.numpy as jnp
from jax import lax

TILE = 256
RANK = 64
SG = 10
GROUPS = 4
ROWS_GRP = 8
NT = 32
NODES = 8192


def draw_columns(key, part):
    row_ids = jnp.arange(NT).astype(jnp.int32)
    group_of = (row_ids // ROWS_GRP)[:, None, None]
    place_of = (row_ids % ROWS_GRP)[:, None, None]
    group_ids = jnp.arange(GROUPS).astype(jnp.int32)[None, :, None]
    offsets = jnp.arange(ROWS_GRP).astype(jnp.int32)[None, None, :]
    allowed = jnp.where(group_ids < group_of, ROWS_GRP, jnp.where(group_ids == group_of, place_of + 1, 0))
    scores = jax.random.randint(jax.random.fold_in(key, 7), (NT, GROUPS, ROWS_GRP), 0, 1 << 20) * ROWS_GRP + offsets
    invalid = (group_ids == group_of) & (offsets > place_of)
    scores = jnp.where(invalid, 1 << 30, scores)
    scores = jnp.where((group_ids == group_of) & (offsets == place_of), -1, scores)
    ordered = jnp.argsort(scores, axis=-1, stable=True).astype(jnp.int32)
    slot_ids = jnp.arange(SG).astype(jnp.int32)
    picked = jnp.take(ordered, jnp.minimum(slot_ids, ROWS_GRP - 1), axis=2)
    live_count = jnp.minimum(allowed[:, :, 0], SG)
    is_live = slot_ids[None, None, :] < live_count[:, :, None]
    group_start = (jnp.arange(GROUPS).astype(jnp.int32) * ROWS_GRP)[None, :, None]
    return jnp.where(is_live, group_start + picked, -1).astype(jnp.int32)


def draw_factor(key, part):
    base = jax.random.uniform(jax.random.fold_in(key, 11), (RANK, NODES), jnp.float32)
    tile_pos = (jnp.arange(NODES) // TILE).astype(jnp.float32) / (NT - 1)
    rising = 1.0 + 0.8 * tile_pos
    values = 0.08 * base * rising[None, :]
    return values.astype(jnp.bfloat16)


def block_levels(rng, dims, cuts, low, largest):
    loudness, own = 1.0, jax.random.fold_in(rng, 6)
    for position, shards_of in cuts:
        steps = jnp.exp(jax.random.uniform(jax.random.fold_in(own, position), (shards_of,), jnp.float32, low / len(cuts), largest / len(cuts)))
        loudness = loudness * jnp.repeat(steps, dims[position] // shards_of).reshape([-1 if axis == position else 1 for axis in range(len(dims))])
    return loudness


def setup_inputs(seed: int = 0) -> dict:
    arg_keys = jax.random.split(jax.random.key(seed), 4)
    blocks = jnp.clip(1.0 * jax.random.uniform(arg_keys[0], (NT, GROUPS, SG, TILE, TILE), jnp.float32) ** block_levels(arg_keys[0], (NT, GROUPS, SG, TILE, TILE), ((0, 32),), -0.2, 0.2), 0.0, 1.0).astype(jnp.bfloat16)
    columns = draw_columns(jax.random.fold_in(arg_keys[3], 71), 0)
    factor = draw_factor(jax.random.fold_in(arg_keys[3], 71), 0)
    return dict(blocks=blocks, columns=columns, factor=factor)


floor_value = 1e-6


def sweep(current, products, gram):
    def update(column, current):
        weights = lax.dynamic_index_in_dim(gram, column, 1, keepdims=False)
        fitted = jnp.dot(weights, current, precision=lax.Precision.HIGHEST)
        target = lax.dynamic_index_in_dim(products, column, 0, keepdims=False)
        present = lax.dynamic_index_in_dim(current, column, 0, keepdims=False)
        diagonal = gram[column, column]
        fresh = jnp.maximum(present + (target - fitted) / diagonal, floor_value)
        return lax.dynamic_update_index_in_dim(current, fresh, column, 0)

    return lax.fori_loop(0, current.shape[0], update, current)


def reference(blocks, columns, factor):
    rank_count, node_count = factor.shape
    tile_size = blocks.shape[-1]
    tile_rows = node_count // tile_size
    slabs = factor.astype(jnp.float32).reshape(rank_count, tile_rows, tile_size).transpose(1, 0, 2)
    row_blocks_all = blocks.reshape(tile_rows, -1, tile_size, tile_size)
    row_cols_all = columns.reshape(tile_rows, -1)

    def one_row(products, inputs):
        row_blocks, row_cols, row_index = inputs
        is_live = (row_cols >= 0).astype(jnp.float32)
        clipped = jnp.where(row_cols >= 0, row_cols, 0).astype(jnp.int32)
        values = row_blocks.astype(jnp.float32)
        fetched = slabs[clipped] * is_live[:, None, None]
        lower_part = jnp.einsum('srv,suv->ru', fetched, values, precision=lax.Precision.HIGHEST)
        own_slab = slabs[row_index]
        mirror = jnp.einsum('ru,suv->srv', own_slab, values, precision=lax.Precision.HIGHEST)
        mirror = mirror * is_live[:, None, None]
        products = products.at[clipped].add(mirror)
        products = products.at[row_index].add(lower_part)
        return products, None

    start_products = jnp.zeros((tile_rows, rank_count, tile_size), jnp.float32)
    indices = jnp.arange(tile_rows).astype(jnp.int32)
    products, _ = lax.scan(one_row, start_products, (row_blocks_all, row_cols_all, indices))
    products = products.transpose(1, 0, 2).reshape(rank_count, node_count)
    gram = jnp.dot(factor, factor.T, preferred_element_type=jnp.float32)
    return sweep(factor.astype(jnp.float32), products, gram)
```

```python
import functools

import jax
import jax.numpy as jnp
from jax import lax
from jax.experimental import pallas as pl
from jax.experimental.pallas import tpu as pltpu
from jax.sharding import PartitionSpec as P

floor_value = 1e-06
VMEM = pl.BlockSpec(memory_space=pltpu.VMEM)
SMEM = pl.BlockSpec(memory_space=pltpu.SMEM)
f32 = jnp.float32
bf16 = jnp.bfloat16


def params(**kw):
    return pltpu.CompilerParams(vmem_limit_bytes=56 * 1024 * 1024, **kw)


def cost(flops, nbytes):
    return pl.CostEstimate(flops=flops, bytes_accessed=nbytes, transcendentals=0)


def mirror_kernel(rows_grp, cols_ref, core_ref, tiles_ref, factor_ref, keep_ref, send_ref, prod):
    h = pl.program_id(0)
    slots = tiles_ref.shape[1]
    core = core_ref[0]
    keep_ref[...] = jnp.zeros_like(keep_ref)
    send_ref[...] = jnp.zeros_like(send_ref)
    own = factor_ref[...]
    for s in range(slots):
        prod[s] = jnp.dot(own, tiles_ref[0, s], preferred_element_type=f32)
    for s in range(slots):
        col = cols_ref[h, s]
        place = col - h * rows_grp
        z = lax.shift_right_arithmetic(place, 1)
        other = jnp.bitwise_and(place, 1) != core

        @pl.when((col >= 0) & other)
        def _():
            send_ref[0, z] = prod[s]

        @pl.when((col >= 0) & jnp.logical_not(other))
        def _():
            keep_ref[0, z] = prod[s]


def mirror(tiles, cols, factor, core, rows_grp):
    groups, all_slots, tile, _ = tiles.shape
    slots = min(all_slots, rows_grp)
    rank = factor.shape[0]
    half = rows_grp // 2
    out = jax.ShapeDtypeStruct((groups, half, rank, tile), f32)
    spec = pl.BlockSpec((1, half, rank, tile), lambda h, *_: (h, 0, 0, 0))
    return pl.pallas_call(
        functools.partial(mirror_kernel, rows_grp),
        grid_spec=pltpu.PrefetchScalarGridSpec(
            num_scalar_prefetch=2,
            grid=(groups,),
            in_specs=[
                pl.BlockSpec((1, slots, tile, tile), lambda h, *_: (h, 0, 0, 0)),
                pl.BlockSpec((rank, tile), lambda h, *_: (0, 0)),
            ],
            out_specs=[spec, spec],
            scratch_shapes=[pltpu.VMEM((slots, rank, tile), f32)],
        ),
        out_shape=[out, out],
        compiler_params=params(),
        cost_estimate=cost(2 * groups * slots * rank * tile * tile, groups * slots * tile * tile * 2),
        name="mirror",
    )(cols, core, tiles, factor)


def split3(value):
    hi = value.astype(bf16)
    rest = value - hi.astype(f32)
    mid = rest.astype(bf16)
    low = (rest - mid.astype(f32)).astype(bf16)
    return hi, mid, low


def pack_kernel(groups, half, where_ref, keep_ref, recv_ref, mine_ref, theirs_ref, rows_ref, own_ref, *pay_refs):
    g, z, core = where_ref[0], where_ref[1], where_ref[2]
    rank = mine_ref.shape[1]
    rows = 2 * half
    gram = jnp.zeros((rank, rank), f32)
    for e in range(half):
        place = 2 * jnp.bitwise_xor(z, e)
        a = mine_ref[e]
        b = theirs_ref[e]
        rows_ref[place + core] = a
        rows_ref[place + 1 - core] = b
        for x in (a, b):
            gram += lax.dot_general(x, x, (((1,), (1,)), ((), ())), preferred_element_type=f32)
    hi, mid, low = split3(gram)
    own_ref[...] = keep_ref[g] + recv_ref[g]
    for d in range(1, groups):
        pay = pay_refs[d - 1]
        t = jnp.bitwise_xor(g, d)
        pay[rows, :, 0:rank] = hi
        pay[rows, :, rank : 2 * rank] = mid
        pay[rows, :, 2 * rank : 3 * rank] = low

        @pl.when(t < g)
        def _():
            for u in range(half):
                value = keep_ref[t, u] + recv_ref[t, u]
                first = value.astype(bf16)
                pay[u] = first
                pay[half + u] = (value - first.astype(f32)).astype(bf16)

        @pl.when(t > g)
        def _():
            pay[0:rows] = rows_ref[...]


def pack(where, keep, recv, mine, theirs):
    groups, half, rank, tile = keep.shape
    rows = 2 * half
    return pl.pallas_call(
        functools.partial(pack_kernel, groups, half),
        in_specs=[SMEM, VMEM, VMEM, VMEM, VMEM],
        out_specs=[VMEM] * (groups + 1),
        out_shape=[
            jax.ShapeDtypeStruct((rows, rank, tile), bf16),
            jax.ShapeDtypeStruct((half, rank, tile), f32),
        ]
        + [jax.ShapeDtypeStruct((rows + 1, rank, tile), bf16)] * (groups - 1),
        compiler_params=params(),
        cost_estimate=cost(2 * rows * rank * rank * tile, keep.size * 8),
        name="pack",
    )(where, keep, recv, mine, theirs)


def merge_kernel(groups, half, where_ref, own_ref, *refs):
    g, z = where_ref[0], where_ref[1]
    arrived = refs[: groups - 1]
    outs = refs[groups - 1 : groups - 1 + half]
    acc = refs[groups - 1 + half]
    acc[...] = own_ref[...]
    for d in range(1, groups):
        src = arrived[d - 1]

        @pl.when(jnp.bitwise_xor(g, d) > g)
        def _():
            acc[...] += src[0:half].astype(f32) + src[half : 2 * half].astype(f32)

    for e in range(half):
        outs[e][...] = acc[jnp.bitwise_xor(z, e)]


def merge(where, own, arrived):
    half, rank, tile = own.shape
    groups = len(arrived) + 1
    return pl.pallas_call(
        functools.partial(merge_kernel, groups, half),
        in_specs=[SMEM, VMEM] + [VMEM] * (groups - 1),
        out_specs=[VMEM] * half,
        out_shape=[jax.ShapeDtypeStruct((rank, tile), f32)] * half,
        scratch_shapes=[pltpu.VMEM((half, rank, tile), f32)],
        compiler_params=params(),
        cost_estimate=cost(own.size * 2 * groups, own.size * 4 * groups),
        name="merge",
    )(where, own, *arrived)


def lower_kernel(groups, rows_grp, cols_ref, where_ref, tiles_ref, rows_ref, *refs):
    arrived = refs[: groups - 1]
    out_ref, gram_ref, held = refs[groups - 1 :]
    h = pl.program_id(0)
    g = where_ref[0]
    slots = tiles_ref.shape[1]
    rank = rows_ref.shape[1]

    @pl.when(h == 0)
    def _():
        out_ref[...] = jnp.zeros_like(out_ref)
        held[rows_grp] = jnp.zeros_like(held[rows_grp])
        gram = jnp.zeros((rank, rank), f32)
        for r in range(rows_grp):
            x = rows_ref[r]
            gram += lax.dot_general(x, x, (((1,), (1,)), ((), ())), preferred_element_type=f32)
        for src in arrived:
            for part in range(3):
                gram += src[rows_grp, :, part * rank : (part + 1) * rank].astype(f32)
        gram_ref[...] = gram

    @pl.when(h == g)
    def _():
        held[0:rows_grp] = rows_ref[...]

    for d in range(1, groups):

        @pl.when((h < g) & (jnp.bitwise_xor(g, d) == h))
        def _():
            held[0:rows_grp] = arrived[d - 1][0:rows_grp]

    @pl.when(h <= g)
    def _():
        total = jnp.zeros(out_ref.shape, f32)
        for s in range(slots):
            col = cols_ref[h, s]
            x = held[jnp.where(col >= 0, col - h * rows_grp, rows_grp)]
            total += lax.dot_general(x, tiles_ref[0, s], (((1,), (1,)), ((), ())), preferred_element_type=f32)
        out_ref[...] += total


def lower(tiles, cols, where, rows, arrived, rows_grp):
    groups, all_slots, tile, _ = tiles.shape
    slots = min(all_slots, rows_grp)
    rank = rows.shape[1]
    whole = lambda shape: pl.BlockSpec(shape, lambda h, *_: (0,) * len(shape))
    return pl.pallas_call(
        functools.partial(lower_kernel, groups, rows_grp),
        grid_spec=pltpu.PrefetchScalarGridSpec(
            num_scalar_prefetch=2,
            grid=(groups,),
            in_specs=[pl.BlockSpec((1, slots, tile, tile), lambda h, *_: (h, 0, 0, 0)), whole(rows.shape)]
            + [whole(x.shape) for x in arrived],
            out_specs=[whole((rank, tile)), whole((rank, rank))],
            scratch_shapes=[pltpu.VMEM((rows_grp + 1, rank, tile), bf16)],
        ),
        out_shape=[jax.ShapeDtypeStruct((rank, tile), f32), jax.ShapeDtypeStruct((rank, rank), f32)],
        compiler_params=params(),
        cost_estimate=cost(2 * groups * slots * rank * tile * tile, groups * slots * tile * tile * 2),
        name="lower",
    )(cols, where, tiles, rows, *arrived)


def sweep_kernel(parts, lower_ref, gram_ref, factor_ref, *refs):
    out_ref = refs[parts]
    rank, tile = factor_ref.shape
    current = factor_ref[...].astype(f32)
    gram = gram_ref[...]
    residual = lower_ref[...]
    for ref in refs[:parts]:
        residual += ref[...]
    residual -= lax.dot_general(
        gram, current, (((0,), (0,)), ((), ())), precision=lax.Precision.HIGHEST, preferred_element_type=f32
    )
    eye = lax.broadcasted_iota(jnp.int32, (rank, rank), 0) == lax.broadcasted_iota(jnp.int32, (rank, rank), 1)
    diagonal = jnp.sum(jnp.where(eye, gram, 0.0), axis=1, keepdims=True)
    inverse = 1.0 / diagonal
    step = 8
    blocks = rank // step
    place = lax.broadcasted_iota(jnp.int32, (step, tile), 0)
    rest = [residual[b * step : (b + 1) * step] for b in range(blocks)]
    for b in range(blocks):
        here = current[b * step : (b + 1) * step]
        inv = jnp.broadcast_to(inverse[b * step : (b + 1) * step], (step, tile))
        result = here
        for k in range(step):
            fresh = jnp.maximum(here + rest[b] * inv, floor_value)
            delta = jnp.broadcast_to((fresh - here)[k : k + 1], (step, tile))
            result = jnp.where(place == k, fresh, result)
            row = b * step + k
            for j in range(b, blocks):
                rest[j] = rest[j] - gram[j * step : (j + 1) * step, row : row + 1] * delta
        out_ref[b * step : (b + 1) * step] = result


def sweep(base, gram, factor, parts):
    rank, tile = factor.shape
    return pl.pallas_call(
        functools.partial(sweep_kernel, len(parts)),
        in_specs=[VMEM] * (3 + len(parts)),
        out_specs=VMEM,
        out_shape=jax.ShapeDtypeStruct((rank, tile), f32),
        compiler_params=params(),
        cost_estimate=cost(2 * rank * rank * tile, rank * tile * 4 * (len(parts) + 3)),
        name="sweep",
    )(base, gram, factor, *parts)


def per_device(blocks, columns, factor):
    tiles = blocks[0]
    cols = columns[0]
    rows_grp = lax.axis_size("row")
    groups = lax.axis_size("grp")
    half = rows_grp // 2
    g = lax.axis_index("grp")
    r = lax.axis_index("row")
    z, core = r // 2, r % 2
    where = jnp.stack([g, z, core]).astype(jnp.int32)
    over_z = lambda x, e: lax.ppermute(x, "row", [(i, ((i // 2) ^ e) * 2 + i % 2) for i in range(rows_grp)])
    over_core = lambda x: lax.ppermute(x, "row", [(i, i ^ 1) for i in range(rows_grp)])
    over_grp = lambda x, d: lax.ppermute(x, "grp", [(i, i ^ d) for i in range(groups)])

    mine = jnp.stack([factor] + [over_z(factor, e) for e in range(1, half)])
    keep, send = mirror(tiles, cols, factor, where[2:3], rows_grp)
    recv = over_core(send)
    theirs = over_core(mine)
    rows, own, *pays = pack(where, keep, recv, mine, theirs)
    arrived = [over_grp(pay, d + 1) for d, pay in enumerate(pays)]
    sums = merge(where, own, arrived)
    final = [sums[0]] + [over_z(sums[e], e) for e in range(1, half)]
    base, gram = lower(tiles, cols, where, rows, arrived, rows_grp)
    return sweep(base, gram, factor, final)


def solution(mesh):
    in_specs = (
        P(("grp", "row"), None, None, None, None),
        P(("grp", "row"), None, None),
        P(None, ("grp", "row")),
    )
    out_specs = P(None, ("grp", "row"))
    return jax.shard_map(
        per_device, mesh=mesh, in_specs=in_specs, out_specs=out_specs, check_vma=False
    )
```

```python
import functools

import jax
import jax.numpy as jnp
from jax import lax
from jax.experimental import pallas as pl
from jax.experimental.pallas import tpu as pltpu
from jax.sharding import PartitionSpec as P

floor_value = 1e-06
VMEM = pl.BlockSpec(memory_space=pltpu.VMEM)
SMEM = pl.BlockSpec(memory_space=pltpu.SMEM)
HBM = pl.BlockSpec(memory_space=pltpu.HBM)
f32 = jnp.float32
bf16 = jnp.bfloat16


def call(kernel, name, in_specs, out_shape, limit, flops, nbytes, scratch=()):
    return pl.pallas_call(
        kernel,
        in_specs=in_specs,
        out_specs=[VMEM] * len(out_shape),
        out_shape=out_shape,
        scratch_shapes=list(scratch),
        compiler_params=pltpu.CompilerParams(vmem_limit_bytes=limit),
        cost_estimate=pl.CostEstimate(flops=flops, bytes_accessed=nbytes, transcendentals=0),
        name=name,
    )


def shape(dims, dtype):
    return jax.ShapeDtypeStruct(dims, dtype)


def dot_nt(a, b):
    return lax.dot_general(a, b, (((1,), (1,)), ((), ())), preferred_element_type=f32)


def mirror_kernel(rows_grp, cols_ref, where_ref, tiles_ref, factor_ref, keep_ref, send_ref, held_ref, stage, sems):
    groups, slots = held_ref.shape[:2]
    half = rows_grp // 2
    rank = factor_ref.shape[0]
    g, core = where_ref[0], where_ref[2]

    def fetch(h):
        return pltpu.make_async_copy(tiles_ref.at[h, pl.ds(0, slots)], held_ref.at[h], sems.at[h])

    for h in range(groups):
        pl.when(h <= g)(lambda: fetch(h).start())
    own = factor_ref[...]
    send_ref[groups * half, :, 0:rank] = dot_nt(own, own)
    for h in range(groups):

        @pl.when(h <= g)
        def _():
            fetch(h).wait()
            stage[...] = jnp.zeros_like(stage)
            for s in range(slots):
                col = cols_ref[h, s]
                place = col - h * rows_grp
                side = jnp.bitwise_xor(jnp.bitwise_and(place, 1), core)
                unit = side * half + lax.shift_right_arithmetic(place, 1)
                unit = jnp.where(col >= 0, unit, 2 * half)
                stage[unit] = jnp.dot(own, held_ref[h, s], preferred_element_type=f32)
            keep_ref[h] = stage[0:half]
            send_ref[h * half : (h + 1) * half] = stage[half : 2 * half]


def mirror(tiles, cols, where, factor, rows_grp):
    groups, all_slots, tile, _ = tiles.shape
    slots = min(all_slots, rows_grp)
    rank = factor.shape[0]
    half = rows_grp // 2
    return call(
        functools.partial(mirror_kernel, rows_grp),
        "mirror",
        [SMEM, SMEM, HBM, VMEM],
        [
            shape((groups, half, rank, tile), f32),
            shape((groups * half + 1, rank, tile), f32),
            shape((groups, slots, tile, tile), bf16),
        ],
        groups * rows_grp * rank * tile * 4 + groups * slots * tile * tile * 2 + (6 << 20),
        2 * groups * slots * rank * tile * tile,
        groups * slots * tile * tile * 2,
        [pltpu.VMEM((2 * half + 1, rank, tile), f32), pltpu.SemaphoreType.DMA((groups,))],
    )(cols, where, tiles, factor)


def split3(value):
    hi = value.astype(bf16)
    rest = value - hi.astype(f32)
    mid = rest.astype(bf16)
    low = (rest - mid.astype(f32)).astype(bf16)
    return hi, mid, low


def pack_kernel(groups, half, where_ref, keep_ref, send_ref, recv_ref, own_ref, *pay_refs):
    g = where_ref[0]
    rank = keep_ref.shape[2]
    last = groups * half
    gram = send_ref[last, :, 0:rank] + recv_ref[last, :, 0:rank]
    parts = split3(gram)
    for u in range(half):
        own_ref[u] = keep_ref[g, u] + recv_ref[g * half + u]
    own_ref[half, :, 0:rank] = gram
    for d in range(1, groups):
        pay = pay_refs[d - 1]
        t = jnp.bitwise_xor(g, d)
        for i, part in enumerate(parts):
            pay[2 * half, :, i * rank : (i + 1) * rank] = part

        @pl.when(t < g)
        def _():
            for u in range(half):
                value = keep_ref[t, u] + recv_ref[t * half + u]
                first = value.astype(bf16)
                pay[u] = first
                pay[half + u] = (value - first.astype(f32)).astype(bf16)


def pack(where, keep, send, recv):
    groups, half, rank, tile = keep.shape
    return call(
        functools.partial(pack_kernel, groups, half),
        "pack",
        [SMEM, VMEM, VMEM, VMEM],
        [shape((half + 1, rank, tile), f32)] + [shape((2 * half + 1, rank, tile), bf16)] * (groups - 1),
        16 << 20,
        keep.size * 4,
        keep.size * 8,
    )(where, keep, send, recv)


def merge_kernel(groups, half, where_ref, own_ref, *refs):
    g, z = where_ref[0], where_ref[1]
    arrived = refs[: groups - 1]
    outs = refs[groups - 1 : groups - 1 + half]
    acc = refs[groups - 1 + half]
    rank, tile = own_ref.shape[1:]
    acc[...] = own_ref[0:half]
    gram = own_ref[half, :, 0:rank]
    for d in range(1, groups):
        src = arrived[d - 1]
        for i in range(3):
            gram += src[2 * half, :, i * rank : (i + 1) * rank].astype(f32)

        @pl.when(jnp.bitwise_xor(g, d) > g)
        def _():
            acc[...] += src[0:half].astype(f32) + src[half : 2 * half].astype(f32)

    extra = outs[0].shape[0] - rank
    for e in range(half):
        outs[e][0:rank] = acc[jnp.bitwise_xor(z, e)]
        for j in range(rank // extra):
            outs[e][rank : rank + extra, j * rank : (j + 1) * rank] = gram[j * extra : (j + 1) * extra]


def merge(where, own, arrived):
    half, rank, tile = own.shape
    half -= 1
    groups = len(arrived) + 1
    return call(
        functools.partial(merge_kernel, groups, half),
        "merge",
        [SMEM, VMEM] + [VMEM] * (groups - 1),
        [shape((rank + rank * rank // tile, tile), f32)] * half,
        16 << 20,
        own.size * 2 * groups,
        own.size * 4 * groups,
        [pltpu.VMEM((half, rank, tile), f32)],
    )(where, own, *arrived)


def lower_kernel(groups, rows_grp, cols_ref, where_ref, tiles_ref, *refs):
    sources = refs[: 2 * groups]
    out_ref, held, acc = refs[2 * groups :]
    slots = tiles_ref.shape[1]
    half = rows_grp // 2
    g, z, core = where_ref[0], where_ref[1], where_ref[2]
    held[groups * rows_grp] = jnp.zeros_like(held[0])
    acc[...] = jnp.zeros_like(acc)
    for d in range(groups):
        t = jnp.bitwise_xor(g, d)

        @pl.when(t <= g)
        def _():
            for side in range(2):
                held[pl.ds(t * rows_grp + side * half, half)] = sources[2 * d + side][...]

    for h in range(groups):

        @pl.when(h <= g)
        def _():
            total = jnp.zeros(acc.shape, f32)
            for s in range(slots):
                col = cols_ref[h, s]
                place = col - h * rows_grp
                side = jnp.bitwise_xor(jnp.bitwise_and(place, 1), core)
                unit = side * half + jnp.bitwise_xor(lax.shift_right_arithmetic(place, 1), z)
                x = held[jnp.where(col >= 0, h * rows_grp + unit, groups * rows_grp)]
                total += dot_nt(tiles_ref[h, s], x)
            acc[...] += total

    out_ref[...] = acc[...].T


def lower(tiles, cols, where, sources, rows_grp):
    groups, slots, tile, _ = tiles.shape
    rank = sources[0].shape[1]
    return call(
        functools.partial(lower_kernel, groups, rows_grp),
        "lower",
        [SMEM, SMEM] + [VMEM] * (1 + len(sources)),
        [shape((rank, tile), f32)],
        20 << 20,
        2 * groups * slots * rank * tile * tile,
        groups * slots * tile * tile * 2,
        [pltpu.VMEM((groups * rows_grp + 1, rank, tile), bf16), pltpu.VMEM((tile, rank), f32)],
    )(cols, where, tiles, *sources)[0]


def sweep_kernel(parts, lower_ref, factor_ref, *refs):
    out_ref = refs[parts]
    rank, tile = factor_ref.shape
    current = factor_ref[...].astype(f32)
    both = refs[0][...]
    for ref in refs[1:parts]:
        both += ref[...]
    extra = both.shape[0] - rank
    gram = jnp.concatenate([both[rank:, j * rank : (j + 1) * rank] for j in range(rank // extra)], axis=0)
    residual = lower_ref[...] + both[:rank]
    residual -= lax.dot_general(
        gram, current, (((0,), (0,)), ((), ())), precision=lax.Precision.HIGHEST, preferred_element_type=f32
    )
    eye = lax.broadcasted_iota(jnp.int32, (rank, rank), 0) == lax.broadcasted_iota(jnp.int32, (rank, rank), 1)
    diagonal = jnp.sum(jnp.where(eye, gram, 0.0), axis=1, keepdims=True)
    inverse = 1.0 / diagonal
    step = 8
    blocks = rank // step
    place = lax.broadcasted_iota(jnp.int32, (step, tile), 0)
    rest = [residual[b * step : (b + 1) * step] for b in range(blocks)]
    for b in range(blocks):
        here = current[b * step : (b + 1) * step]
        inv = jnp.broadcast_to(inverse[b * step : (b + 1) * step], (step, tile))
        result = here
        for k in range(step):
            fresh = jnp.maximum(here + rest[b] * inv, floor_value)
            delta = jnp.broadcast_to((fresh - here)[k : k + 1], (step, tile))
            result = jnp.where(place == k, fresh, result)
            row = b * step + k
            for j in range(b, blocks):
                rest[j] = rest[j] - gram[j * step : (j + 1) * step, row : row + 1] * delta
        out_ref[b * step : (b + 1) * step] = result


def sweep(base, factor, parts):
    rank, tile = factor.shape
    return call(
        functools.partial(sweep_kernel, len(parts)),
        "sweep",
        [VMEM] * (2 + len(parts)),
        [shape((rank, tile), f32)],
        8 << 20,
        2 * rank * rank * tile,
        rank * tile * 4 * (len(parts) + 3),
    )(base, factor, *parts)[0]


def per_device(blocks, columns, factor):
    tiles = pltpu.with_memory_space_constraint(blocks[0], pltpu.HBM)
    cols = pltpu.with_memory_space_constraint(columns[0], pltpu.HBM)
    rows_grp = lax.axis_size("row")
    groups = lax.axis_size("grp")
    half = rows_grp // 2
    g = lax.axis_index("grp")
    r = lax.axis_index("row")
    where = jnp.stack([g, r // 2, r % 2]).astype(jnp.int32)
    over_z = lambda x, e: lax.ppermute(x, "row", [(i, ((i // 2) ^ e) * 2 + i % 2) for i in range(rows_grp)])
    over_core = lambda x: lax.ppermute(x, "row", [(i, i ^ 1) for i in range(rows_grp)])
    over_grp = lambda x, d: lax.ppermute(x, "grp", [(i, i ^ d) for i in range(groups)])
    up_grp = lambda x, d: lax.ppermute(x, "grp", [(i, i ^ d) for i in range(groups) if i ^ d > i])

    keep, send, held = mirror(tiles, cols, where, factor, rows_grp)
    recv = over_core(send)
    own, *pays = pack(where, keep, send, recv)
    arrived = [over_grp(pay, d + 1) for d, pay in enumerate(pays)]
    sums = merge(where, own, arrived)
    final = [sums[0]] + [over_z(sums[e], e) for e in range(1, half)]

    mine = jnp.stack([factor] + [over_z(factor, e) for e in range(1, half)])
    rows = [mine] + [up_grp(mine, d) for d in range(1, groups)]
    sources = [x for block in rows for x in (block, over_core(block))]
    base = lower(held, cols, where, sources, rows_grp)
    return sweep(base, factor, final)


def solution(mesh):
    in_specs = (
        P(("grp", "row"), None, None, None, None),
        P(("grp", "row"), None, None),
        P(None, ("grp", "row")),
    )
    out_specs = P(None, ("grp", "row"))
    return jax.shard_map(
        per_device, mesh=mesh, in_specs=in_specs, out_specs=out_specs, check_vma=False
    )
```

```python
import functools

import jax
import jax.numpy as jnp
from jax import lax
from jax.experimental import pallas as pl
from jax.experimental.pallas import tpu as pltpu
from jax.sharding import PartitionSpec as P

floor_value = 1e-06
VMEM = pl.BlockSpec(memory_space=pltpu.VMEM)
SMEM = pl.BlockSpec(memory_space=pltpu.SMEM)
HBM = pl.BlockSpec(memory_space=pltpu.HBM)
f32 = jnp.float32
bf16 = jnp.bfloat16


def call(kernel, name, in_specs, out_shape, limit, flops, nbytes, scratch=()):
    return pl.pallas_call(
        kernel,
        in_specs=in_specs,
        out_specs=[VMEM] * len(out_shape),
        out_shape=out_shape,
        scratch_shapes=list(scratch),
        compiler_params=pltpu.CompilerParams(vmem_limit_bytes=limit),
        cost_estimate=pl.CostEstimate(flops=flops, bytes_accessed=nbytes, transcendentals=0),
        name=name,
    )


def shape(dims, dtype):
    return jax.ShapeDtypeStruct(dims, dtype)


def dot_nt(a, b):
    return lax.dot_general(a, b, (((1,), (1,)), ((), ())), preferred_element_type=f32)


def mirror_kernel(rows_grp, cols_ref, where_ref, tiles_ref, factor_ref, keep_ref, send_ref, held_ref, stage, sems):
    groups, slots = held_ref.shape[:2]
    half = rows_grp // 2
    g, core = where_ref[0], where_ref[2]

    def fetch(h):
        return pltpu.make_async_copy(tiles_ref.at[h, pl.ds(0, slots)], held_ref.at[h], sems.at[h])

    for h in range(groups):
        pl.when(h <= g)(lambda: fetch(h).start())
    own = factor_ref[...]
    for h in range(groups):

        @pl.when(h <= g)
        def _():
            fetch(h).wait()
            stage[...] = jnp.zeros_like(stage)
            for s in range(slots):
                col = cols_ref[h, s]
                place = col - h * rows_grp
                side = jnp.bitwise_xor(jnp.bitwise_and(place, 1), core)
                unit = side * half + lax.shift_right_arithmetic(place, 1)
                unit = jnp.where(col >= 0, unit, 2 * half)
                stage[unit] = jnp.dot(own, held_ref[h, s], preferred_element_type=f32)
            keep_ref[h] = stage[0:half]
            send_ref[h] = stage[half : 2 * half]


def mirror(tiles, cols, where, factor, rows_grp):
    groups, all_slots, tile, _ = tiles.shape
    slots = min(all_slots, rows_grp)
    rank = factor.shape[0]
    half = rows_grp // 2
    return call(
        functools.partial(mirror_kernel, rows_grp),
        "mirror",
        [SMEM, SMEM, HBM, VMEM],
        [shape((groups, half, rank, tile), f32)] * 2 + [shape((groups, slots, tile, tile), bf16)],
        groups * rows_grp * rank * tile * 4 + groups * slots * tile * tile * 2 + (6 << 20),
        2 * groups * slots * rank * tile * tile,
        groups * slots * tile * tile * 2,
        [pltpu.VMEM((2 * half + 1, rank, tile), f32), pltpu.SemaphoreType.DMA((groups,))],
    )(cols, where, tiles, factor)


LOWEST = -64
LADDER = (64, 32, 16, 8, 4, 2, 1)


def row_scale(top):
    power = jnp.full(top.shape, 2.0**LOWEST, f32)
    inverse = jnp.full(top.shape, 2.0**-LOWEST, f32)
    steps = jnp.zeros(top.shape, jnp.int32)
    for b in LADDER:
        up = top >= power * 2.0**b
        power = jnp.where(up, power * 2.0**b, power)
        inverse = jnp.where(up, inverse * 2.0**-b, inverse)
        steps = jnp.where(up, steps + b, steps)
    return inverse, steps


def row_power(steps):
    power = jnp.full(steps.shape, 2.0**LOWEST, f32)
    for b in LADDER:
        power = jnp.where(jnp.bitwise_and(steps, b) != 0, power * 2.0**b, power)
    return power


def encode(pay, values):
    rank = values[0].shape[0]
    mid = rank // 2
    top = functools.reduce(jnp.maximum, values)
    inverse, steps = row_scale(jnp.max(top, axis=1, keepdims=True))
    factor = inverse * 2.0**15
    for u, value in enumerate(values):
        q = jnp.minimum((value * factor + 0.5).astype(jnp.int32), 65535)
        pay[u * mid : (u + 1) * mid] = jnp.bitwise_or(q[:mid], lax.shift_left(q[mid:], 16))
    put_block(pay, steps, 96, 32)


def decode(pay, u, power):
    mid = power.shape[0] // 2
    word = pay[u * mid : (u + 1) * mid]
    low = jnp.bitwise_and(word, 65535).astype(f32)
    high = jnp.bitwise_and(lax.shift_right_logical(word, 16), 65535).astype(f32)
    return jnp.concatenate([low, high], axis=0) * power


def put_block(pay, value, lane, width):
    mid = value.shape[0] // 2
    base = pay.shape[0] - mid
    value = jnp.broadcast_to(value, (2 * mid, width))
    pay[base:, lane : lane + width] = value[:mid]
    pay[base:, 128 + lane : 128 + lane + width] = value[mid:]


def get_block(pay, mid, lane, width):
    base = pay.shape[0] - mid
    return jnp.concatenate([pay[base:, lane : lane + width], pay[base:, 128 + lane : 128 + lane + width]], axis=0)


def pack_kernel(groups, half, where_ref, keep_ref, recv_ref, *refs):
    rows, outs = refs[:half], refs[half:]
    own_ref, mine_ref, gram_ref = outs[:3]
    g = where_ref[0]
    rank = keep_ref.shape[2]
    gram = jnp.zeros((rank, rank), f32)
    for e in range(half):
        mine_ref[e] = rows[e][...]
        gram += dot_nt(rows[e][...], rows[e][...])
    gram_ref[...] = gram
    inverse, steps = row_scale(jnp.max(gram, axis=1, keepdims=True))
    coded = (gram * (inverse * 2.0**29) + 0.5).astype(jnp.int32)
    own_ref[...] = keep_ref[g] + recv_ref[g]
    for d in range(1, groups):
        pay = outs[2 + d]
        t = jnp.bitwise_xor(g, d)
        put_block(pay, coded, 0, rank)
        put_block(pay, steps, 64, 32)

        @pl.when(t < g)
        def _():
            encode(pay, [keep_ref[t, u] + recv_ref[t, u] for u in range(half)])

        @pl.when(t > g)
        def _():
            encode(pay, [rows[u][...].astype(f32) for u in range(half)])


def pack(where, keep, recv, rows):
    groups, half, rank, tile = keep.shape
    return call(
        functools.partial(pack_kernel, groups, half),
        "pack",
        [SMEM, VMEM, VMEM] + [VMEM] * half,
        [shape((half, rank, tile), f32), shape((half, rank, tile), bf16), shape((rank, rank), f32)]
        + [shape(((half + 1) * rank // 2, tile), jnp.int32)] * (groups - 1),
        16 << 20,
        keep.size * 4,
        keep.size * 8,
    )(where, keep, recv, *rows)


def split3(value):
    hi = value.astype(bf16)
    rest = value - hi.astype(f32)
    mid = rest.astype(bf16)
    low = (rest - mid.astype(f32)).astype(bf16)
    return hi, mid, low


def merge_kernel(groups, half, where_ref, own_ref, gram_ref, *refs):
    g, z = where_ref[0], where_ref[1]
    arrived = refs[: groups - 1]
    outs = refs[groups - 1 : groups - 1 + half]
    heard_ref, total_ref, acc = refs[groups - 1 + half :]
    rank = own_ref.shape[1]
    acc[...] = own_ref[...]
    gram = gram_ref[...]
    for d in range(1, groups):
        pay = arrived[d - 1]
        power = row_power(get_block(pay, rank // 2, 64, 1)) * 2.0**-29
        gram += get_block(pay, rank // 2, 0, rank).astype(f32) * power
        power = row_power(get_block(pay, rank // 2, 96, 1)) * 2.0**-15
        s = jnp.bitwise_xor(g, d)

        @pl.when(s > g)
        def _():
            for u in range(half):
                acc[u] += decode(pay, u, power)

        @pl.when(s < g)
        def _():
            for u in range(half):
                heard_ref[(d - 1) * half + u] = decode(pay, u, power).astype(bf16)

    total_ref[...] = gram
    for i, part in enumerate(split3(gram)):
        heard_ref[(groups - 1) * half, :, i * rank : (i + 1) * rank] = part
    for e in range(half):
        outs[e][...] = acc[jnp.bitwise_xor(z, e)]


def merge(where, own, gram, arrived):
    half, rank, tile = own.shape
    groups = len(arrived) + 1
    return call(
        functools.partial(merge_kernel, groups, half),
        "merge",
        [SMEM, VMEM, VMEM] + [VMEM] * (groups - 1),
        [shape((rank, tile), f32)] * half
        + [shape(((groups - 1) * half + 1, rank, tile), bf16), shape((rank, rank), f32)],
        16 << 20,
        own.size * 2 * groups,
        own.size * 4 * groups,
        [pltpu.VMEM((half, rank, tile), f32)],
    )(where, own, gram, *arrived)


def lower_kernel(groups, rows_grp, cols_ref, where_ref, tiles_ref, factor_ref, part_ref, *refs):
    mine_ref, theirs_ref, heard_ref, told_ref, out_ref, gram_ref, held, acc = refs
    slots = tiles_ref.shape[1]
    half = rows_grp // 2
    rank = factor_ref.shape[0]
    g, z, core = where_ref[0], where_ref[1], where_ref[2]
    held[groups * rows_grp] = jnp.zeros_like(held[0])
    held[pl.ds(g * rows_grp, half)] = mine_ref[...]
    held[pl.ds(g * rows_grp + half, half)] = theirs_ref[...]
    for d in range(1, groups):
        t = jnp.bitwise_xor(g, d)

        @pl.when(t < g)
        def _():
            held[pl.ds(t * rows_grp, half)] = heard_ref[(d - 1) * half : d * half]
            held[pl.ds(t * rows_grp + half, half)] = told_ref[(d - 1) * half : d * half]

    gram = part_ref[...]
    for i in range(3):
        gram += told_ref[(groups - 1) * half, :, i * rank : (i + 1) * rank].astype(f32)
    gram_ref[...] = gram
    acc[...] = jnp.zeros_like(acc)
    for h in range(groups):

        @pl.when(h <= g)
        def _():
            total = jnp.zeros(acc.shape, f32)
            for s in range(slots):
                col = cols_ref[h, s]
                place = col - h * rows_grp
                side = jnp.bitwise_xor(jnp.bitwise_and(place, 1), core)
                unit = side * half + jnp.bitwise_xor(lax.shift_right_arithmetic(place, 1), z)
                x = held[jnp.where(col >= 0, h * rows_grp + unit, groups * rows_grp)]
                total += dot_nt(tiles_ref[h, s], x)
            acc[...] += total

    fitted = lax.dot_general(
        gram,
        factor_ref[...].astype(f32),
        (((0,), (0,)), ((), ())),
        precision=lax.Precision.HIGHEST,
        preferred_element_type=f32,
    )
    out_ref[...] = acc[...].T - fitted


def lower(tiles, cols, where, factor, part, sources, rows_grp):
    groups, slots, tile, _ = tiles.shape
    rank = factor.shape[0]
    return call(
        functools.partial(lower_kernel, groups, rows_grp),
        "lower",
        [SMEM, SMEM] + [VMEM] * (3 + len(sources)),
        [shape((rank, tile), f32), shape((rank, rank), f32)],
        20 << 20,
        2 * groups * slots * rank * tile * tile,
        groups * slots * tile * tile * 2,
        [pltpu.VMEM((groups * rows_grp + 1, rank, tile), bf16), pltpu.VMEM((tile, rank), f32)],
    )(cols, where, tiles, factor, part, *sources)


def sweep_kernel(parts, base_ref, gram_ref, factor_ref, *refs):
    out_ref = refs[parts]
    rank, tile = factor_ref.shape
    current = factor_ref[...].astype(f32)
    gram = gram_ref[...]
    residual = base_ref[...]
    for ref in refs[:parts]:
        residual += ref[...]
    eye = lax.broadcasted_iota(jnp.int32, (rank, rank), 0) == lax.broadcasted_iota(jnp.int32, (rank, rank), 1)
    diagonal = jnp.sum(jnp.where(eye, gram, 0.0), axis=1, keepdims=True)
    inverse = 1.0 / diagonal
    step = 8
    blocks = rank // step
    place = lax.broadcasted_iota(jnp.int32, (step, tile), 0)
    rest = [residual[b * step : (b + 1) * step] for b in range(blocks)]
    for b in range(blocks):
        here = current[b * step : (b + 1) * step]
        inv = jnp.broadcast_to(inverse[b * step : (b + 1) * step], (step, tile))
        result = here
        for k in range(step):
            fresh = jnp.maximum(here + rest[b] * inv, floor_value)
            delta = jnp.broadcast_to((fresh - here)[k : k + 1], (step, tile))
            result = jnp.where(place == k, fresh, result)
            row = b * step + k
            for j in range(b, blocks):
                rest[j] = rest[j] - gram[j * step : (j + 1) * step, row : row + 1] * delta
        out_ref[b * step : (b + 1) * step] = result


def sweep(base, gram, factor, parts):
    rank, tile = factor.shape
    return call(
        functools.partial(sweep_kernel, len(parts)),
        "sweep",
        [VMEM] * (3 + len(parts)),
        [shape((rank, tile), f32)],
        8 << 20,
        2 * rank * rank * tile,
        rank * tile * 4 * (len(parts) + 3),
    )(base, gram, factor, *parts)[0]


def per_device(blocks, columns, factor):
    tiles = pltpu.with_memory_space_constraint(blocks[0], pltpu.HBM)
    cols = pltpu.with_memory_space_constraint(columns[0], pltpu.HBM)
    rows_grp = lax.axis_size("row")
    groups = lax.axis_size("grp")
    half = rows_grp // 2
    g = lax.axis_index("grp")
    r = lax.axis_index("row")
    where = jnp.stack([g, r // 2, r % 2]).astype(jnp.int32)
    over_z = lambda x, e: lax.ppermute(x, "row", [(i, ((i // 2) ^ e) * 2 + i % 2) for i in range(rows_grp)])
    over_core = lambda x: lax.ppermute(x, "row", [(i, i ^ 1) for i in range(rows_grp)])
    over_grp = lambda x, d: lax.ppermute(x, "grp", [(i, i ^ d) for i in range(groups)])

    rows = [factor] + [over_z(factor, e) for e in range(1, half)]
    keep, send, held = mirror(tiles, cols, where, factor, rows_grp)
    recv = over_core(send)
    own, mine, gram, *pays = pack(where, keep, recv, rows)
    arrived = [over_grp(pay, d + 1) for d, pay in enumerate(pays)]
    theirs = over_core(mine)
    *sums, heard, part = merge(where, own, gram, arrived)
    final = [sums[0]] + [over_z(sums[e], e) for e in range(1, half)]
    told = over_core(heard)
    base, gram = lower(held, cols, where, factor, part, [mine, theirs, heard, told], rows_grp)
    return sweep(base, gram, factor, final)


def solution(mesh):
    in_specs = (
        P(("grp", "row"), None, None, None, None),
        P(("grp", "row"), None, None),
        P(None, ("grp", "row")),
    )
    out_specs = P(None, ("grp", "row"))
    return jax.shard_map(
        per_device, mesh=mesh, in_specs=in_specs, out_specs=out_specs, check_vma=False
    )
```

```python
import functools

import jax
import jax.numpy as jnp
from jax import lax
from jax.experimental import pallas as pl
from jax.experimental.pallas import tpu as pltpu
from jax.sharding import PartitionSpec as P


floor_value = 1e-06
VMEM = pl.BlockSpec(memory_space=pltpu.VMEM)
SMEM = pl.BlockSpec(memory_space=pltpu.SMEM)
HBM = pl.BlockSpec(memory_space=pltpu.HBM)
f32 = jnp.float32
bf16 = jnp.bfloat16


def call(kernel, in_specs, out_shape, limit, flops, nbytes, scratch=()):
    return pl.pallas_call(
        kernel,
        in_specs=in_specs,
        out_specs=[VMEM] * len(out_shape),
        out_shape=out_shape,
        scratch_shapes=list(scratch),
        compiler_params=pltpu.CompilerParams(vmem_limit_bytes=limit),
        cost_estimate=pl.CostEstimate(flops=flops, bytes_accessed=nbytes, transcendentals=0),
    )


def shape(dims, dtype):
    return jax.ShapeDtypeStruct(dims, dtype)


def dot_nt(a, b):
    return lax.dot_general(a, b, (((1,), (1,)), ((), ())), preferred_element_type=f32)


def position():
    r = lax.axis_index("row")
    return lax.axis_index("grp"), lax.shift_right_logical(r, 1), jnp.bitwise_and(r, 1)


def ahead_kernel(zero_ref):
    zero_ref[...] = jnp.zeros_like(zero_ref)


def ahead(dims):
    return call(ahead_kernel, [], [shape(dims, f32)], 1 << 20, 8 << 30, 24 << 20)()[0]


def mirror_kernel(rows_grp, cols_ref, tiles_ref, factor_ref, zero_ref, keep_ref, send_ref, stage):
    groups = tiles_ref.shape[0]
    half = rows_grp // 2
    slots = min(tiles_ref.shape[1], rows_grp)
    g, _, core = position()
    own = factor_ref[...]
    for h in range(groups):

        @pl.when(h <= g)
        def _():
            for u in range(2 * half):
                stage[u] = zero_ref[...]
            for s in range(slots):
                col = cols_ref[h, s]
                place = col - h * rows_grp
                side = jnp.bitwise_xor(jnp.bitwise_and(place, 1), core)
                unit = side * half + lax.shift_right_arithmetic(place, 1)
                unit = jnp.where(col >= 0, unit, 2 * half)
                stage[unit] = jnp.dot(own, tiles_ref[h, s], preferred_element_type=f32)
            keep_ref[h] = stage[0:half]
            send_ref[h] = stage[half : 2 * half]


def mirror(tiles, cols, factor, zero, rows_grp):
    groups, slots, tile, _ = tiles.shape
    rank = factor.shape[0]
    half = rows_grp // 2
    return call(
        functools.partial(mirror_kernel, rows_grp),
        [SMEM, VMEM, VMEM, VMEM],
        [shape((groups, half, rank, tile), f32)] * 2,
        12 << 20,
        2 * groups * slots * rank * tile * tile,
        groups * slots * tile * tile * 2,
        [pltpu.VMEM((2 * half + 1, rank, tile), f32)],
    )(cols, tiles, factor, zero)


LOWEST = -64
LADDER = (64, 32, 16, 8, 4, 2, 1)


def row_scale(top):
    power = jnp.full(top.shape, 2.0**LOWEST, f32)
    inverse = jnp.full(top.shape, 2.0**-LOWEST, f32)
    steps = jnp.zeros(top.shape, jnp.int32)
    for b in LADDER:
        up = top >= power * 2.0**b
        power = jnp.where(up, power * 2.0**b, power)
        inverse = jnp.where(up, inverse * 2.0**-b, inverse)
        steps = jnp.where(up, steps + b, steps)
    return inverse, steps


def row_power(steps):
    power = jnp.full(steps.shape, 2.0**LOWEST, f32)
    for b in LADDER:
        power = jnp.where(jnp.bitwise_and(steps, b) != 0, power * 2.0**b, power)
    return power


def encode(pay, values):
    rank = values[0].shape[0]
    mid = rank // 2
    top = functools.reduce(jnp.maximum, values)
    inverse, steps = row_scale(jnp.max(top, axis=1, keepdims=True))
    factor = inverse * 2.0**15
    for u, value in enumerate(values):
        q = jnp.minimum((value * factor + 0.5).astype(jnp.int32), 65535)
        pay[u * mid : (u + 1) * mid] = jnp.bitwise_or(q[:mid], lax.shift_left(q[mid:], 16))
    return steps


def decode(pay, u, power):
    mid = power.shape[0] // 2
    word = pay[u * mid : (u + 1) * mid]
    low = jnp.bitwise_and(word, 65535).astype(f32)
    high = jnp.bitwise_and(lax.shift_right_logical(word, 16), 65535).astype(f32)
    return jnp.concatenate([low, high], axis=0) * power


def put_steps(pay, *several):
    rank = several[0].shape[0]
    base, wide = pay.shape[0] - 8, pay.shape[1] * 8 // rank
    lanes = wide // len(several)
    for j, steps in enumerate(several):
        for i in range(rank // 8):
            at = i * wide + j * lanes
            pay[base:, at : at + lanes] = jnp.broadcast_to(steps[i * 8 : i * 8 + 8], (8, lanes))


def get_steps(pay, rank, j, of):
    base, wide = pay.shape[0] - 8, pay.shape[1] * 8 // rank
    at = [i * wide + j * (wide // of) for i in range(rank // 8)]
    return jnp.concatenate([pay[base:, k : k + 1] for k in at], axis=0)


def put_square(pay, base, square):
    rank = square.shape[0]
    rows = rank * rank // pay.shape[1]
    for j in range(rank // rows):
        pay[base : base + rows, j * rank : (j + 1) * rank] = square[j * rows : (j + 1) * rows]


def get_square(pay, base, rank):
    rows = rank * rank // pay.shape[1]
    return jnp.concatenate([pay[base : base + rows, j * rank : (j + 1) * rank] for j in range(rank // rows)], axis=0)


def pack_kernel(groups, half, keep_ref, recv_ref, *refs):
    rows, outs = refs[:half], refs[half:]
    own_ref, mine_ref, gram_ref = outs[:3]
    g, _, _ = position()
    rank = keep_ref.shape[2]
    gram = jnp.zeros((rank, rank), f32)
    for e in range(half):
        mine_ref[e] = rows[e][...]
        gram += dot_nt(rows[e][...], rows[e][...])
    gram_ref[...] = gram
    inverse, steps = row_scale(jnp.max(gram, axis=1, keepdims=True))
    coded = (gram * (inverse * 2.0**29) + 0.5).astype(jnp.int32)
    own_ref[...] = keep_ref[g] + recv_ref[g]
    for d in range(1, groups):
        pay = outs[2 + d]
        t = jnp.bitwise_xor(g, d)
        put_square(pay, half * rank // 2, coded)
        down = t < g
        sums = [keep_ref[t, u] + recv_ref[t, u] for u in range(half)]
        above = encode(pay, [jnp.where(down, sums[u], rows[u][...].astype(f32)) for u in range(half)])
        put_steps(pay, above, steps)


def pack(keep, recv, rows):
    groups, half, rank, tile = keep.shape
    return call(
        functools.partial(pack_kernel, groups, half),
        [VMEM, VMEM] + [VMEM] * half,
        [shape((half, rank, tile), f32), shape((half, rank, tile), bf16), shape((rank, rank), f32)]
        + [shape((half * rank // 2 + rank * rank // tile + 8, tile), jnp.int32)] * (groups - 1),
        16 << 20,
        keep.size * 4,
        keep.size * 8,
    )(keep, recv, *rows)


def split3(value):
    hi = value.astype(bf16)
    rest = value - hi.astype(f32)
    mid = rest.astype(bf16)
    low = (rest - mid.astype(f32)).astype(bf16)
    return hi, mid, low


def merge_kernel(groups, half, own_ref, gram_ref, *refs):
    g, z, _ = position()
    arrived = refs[: groups - 1]
    outs = refs[groups - 1 : groups - 1 + half]
    heard_ref, total_ref, acc = refs[groups - 1 + half :]
    rank = own_ref.shape[1]
    gram = gram_ref[...]
    sums = [own_ref[u] for u in range(half)]
    for d in range(1, groups):
        pay = arrived[d - 1]
        power = row_power(get_steps(pay, rank, 1, 2)) * 2.0**-29
        gram += get_square(pay, half * rank // 2, rank).astype(f32) * power
        power = row_power(get_steps(pay, rank, 0, 2)) * 2.0**-15
        above = jnp.bitwise_xor(g, d) > g
        for u in range(half):
            value = decode(pay, u, power)
            sums[u] += jnp.where(above, value, 0.0)
            heard_ref[(d - 1) * half + u] = value.astype(bf16)

    total_ref[...] = gram
    for i, part in enumerate(split3(gram)):
        heard_ref[(groups - 1) * half, :, i * rank : (i + 1) * rank] = part
    for u in range(half):
        acc[u] = sums[u]
    outs[0][...] = acc[z]
    for e in range(1, half):
        put_steps(outs[e], encode(outs[e], [acc[jnp.bitwise_xor(z, e)]]))


def merge(own, gram, arrived):
    half, rank, tile = own.shape
    groups = len(arrived) + 1
    return call(
        functools.partial(merge_kernel, groups, half),
        [VMEM, VMEM] + [VMEM] * (groups - 1),
        [shape((rank, tile), f32)]
        + [shape((rank // 2 + 8, tile), jnp.int32)] * (half - 1)
        + [shape(((groups - 1) * half + 1, rank, tile), bf16), shape((rank, rank), f32)],
        16 << 20,
        own.size * 2 * groups,
        own.size * 4 * groups,
        [pltpu.VMEM((half, rank, tile), f32)],
    )(own, gram, *arrived)


def row_products(cols_ref, tiles_ref, held, h, base, rows_grp):
    _, z, core = position()
    half = rows_grp // 2
    total = None
    for s in range(min(tiles_ref.shape[1], rows_grp)):
        col = cols_ref[h, s]
        place = col - h * rows_grp
        side = jnp.bitwise_xor(jnp.bitwise_and(place, 1), core)
        unit = side * half + jnp.bitwise_xor(lax.shift_right_arithmetic(place, 1), z)
        x = held[jnp.where(col >= 0, base + unit, held.shape[0] - 1)]
        term = dot_nt(tiles_ref[h, s], x)
        total = term if total is None else total + term
    return total


def near_kernel(rows_grp, cols_ref, tiles_ref, mine_ref, theirs_ref, out_ref, held):
    g, _, _ = position()
    half = rows_grp // 2
    held[0:half] = mine_ref[...]
    held[half:rows_grp] = theirs_ref[...]
    held[rows_grp] = jnp.zeros_like(held[0])
    out_ref[...] = row_products(cols_ref, tiles_ref, held, g, 0, rows_grp)


def near(tiles, cols, mine, theirs, rows_grp):
    _, slots, tile, _ = tiles.shape
    rank = mine.shape[1]
    return call(
        functools.partial(near_kernel, rows_grp),
        [SMEM, VMEM, VMEM, VMEM],
        [shape((tile, rank), f32)],
        8 << 20,
        2 * slots * rank * tile * tile,
        slots * tile * tile * 2,
        [pltpu.VMEM((rows_grp + 1, rank, tile), bf16)],
    )(cols, tiles, mine, theirs)[0]


def lower_kernel(groups, rows_grp, cols_ref, tiles_ref, factor_ref, near_ref, part_ref, *refs):
    heard_ref, told_ref, out_ref, gram_ref, held, acc = refs
    half = rows_grp // 2
    rank = factor_ref.shape[0]
    g, _, _ = position()
    held[groups * rows_grp] = jnp.zeros_like(held[0])
    for d in range(1, groups):
        t = jnp.bitwise_xor(g, d)
        held[pl.ds(t * rows_grp, half)] = heard_ref[(d - 1) * half : d * half]
        held[pl.ds(t * rows_grp + half, half)] = told_ref[(d - 1) * half : d * half]

    gram = part_ref[...]
    for i in range(3):
        gram += told_ref[(groups - 1) * half, :, i * rank : (i + 1) * rank].astype(f32)
    gram_ref[...] = gram
    acc[...] = near_ref[...]
    for h in range(groups - 1):

        @pl.when(h < g)
        def _():
            acc[...] += row_products(cols_ref, tiles_ref, held, h, h * rows_grp, rows_grp)

    fitted = lax.dot_general(
        gram,
        factor_ref[...].astype(f32),
        (((0,), (0,)), ((), ())),
        precision=lax.Precision.HIGHEST,
        preferred_element_type=f32,
    )
    out_ref[...] = acc[...].T - fitted


def lower(tiles, cols, factor, first, part, heard, told, rows_grp):
    groups, slots, tile, _ = tiles.shape
    rank = factor.shape[0]
    return call(
        functools.partial(lower_kernel, groups, rows_grp),
        [SMEM] + [VMEM] * 6,
        [shape((rank, tile), f32), shape((rank, rank), f32)],
        20 << 20,
        2 * groups * slots * rank * tile * tile,
        groups * slots * tile * tile * 2,
        [pltpu.VMEM((groups * rows_grp + 1, rank, tile), bf16), pltpu.VMEM((tile, rank), f32)],
    )(cols, tiles, factor, first, part, heard, told)


def sweep_kernel(parts, base_ref, gram_ref, factor_ref, own_ref, *refs):
    out_ref = refs[parts]
    rank, tile = factor_ref.shape
    current = factor_ref[...].astype(f32)
    gram = gram_ref[...]
    residual = base_ref[...] + own_ref[...]
    for ref in refs[:parts]:
        residual += decode(ref, 0, row_power(get_steps(ref, rank, 0, 1)) * 2.0**-15)
    eye = lax.broadcasted_iota(jnp.int32, (rank, rank), 0) == lax.broadcasted_iota(jnp.int32, (rank, rank), 1)
    diagonal = jnp.sum(jnp.where(eye, gram, 0.0), axis=1, keepdims=True)
    inverse = 1.0 / diagonal
    step = 8
    blocks = rank // step
    place = lax.broadcasted_iota(jnp.int32, (step, tile), 0)
    rest = [residual[b * step : (b + 1) * step] for b in range(blocks)]
    for b in range(blocks):
        here = current[b * step : (b + 1) * step]
        inv = jnp.broadcast_to(inverse[b * step : (b + 1) * step], (step, tile))
        result = here
        for k in range(step):
            fresh = jnp.maximum(here + rest[b] * inv, floor_value)
            delta = jnp.broadcast_to((fresh - here)[k : k + 1], (step, tile))
            result = jnp.where(place == k, fresh, result)
            row = b * step + k
            for j in range(b, blocks):
                rest[j] = rest[j] - gram[j * step : (j + 1) * step, row : row + 1] * delta
        out_ref[b * step : (b + 1) * step] = result


def sweep(base, gram, factor, own, parts):
    rank, tile = factor.shape
    return call(
        functools.partial(sweep_kernel, len(parts)),
        [VMEM] * (4 + len(parts)),
        [shape((rank, tile), f32)],
        8 << 20,
        2 * rank * rank * tile,
        rank * tile * 4 * (len(parts) + 3),
    )(base, gram, factor, own, *parts)[0]


def per_device(blocks, columns, factor):
    tiles = blocks[0]
    cols = pltpu.with_memory_space_constraint(columns[0], pltpu.HBM)
    rows_grp = lax.axis_size("row")
    groups = lax.axis_size("grp")
    half = rows_grp // 2

    def over_z(x, e):
        return lax.ppermute(x, "row", [(i, ((i // 2) ^ e) * 2 + i % 2) for i in range(rows_grp)])

    def over_core(x):
        return lax.ppermute(x, "row", [(i, i ^ 1) for i in range(rows_grp)])

    def over_grp(x, d):
        return lax.ppermute(x, "grp", [(i, i ^ d) for i in range(groups)])

    zero = ahead(factor.shape)
    rows = [factor]
    for e in range(1, half):
        low = e & -e
        rows.append(over_z(rows[e - low], low))
    keep, send = mirror(tiles, cols, factor, zero, rows_grp)
    recv = over_core(send)
    own, mine, gram, *pays = pack(keep, recv, rows)
    arrived = [over_grp(pay, d + 1) for d, pay in enumerate(pays)]
    theirs = over_core(mine)
    first = near(tiles, cols, mine, theirs, rows_grp)
    *sums, heard, part = merge(own, gram, arrived)
    told = over_core(heard)
    parts = [over_z(sums[e], e) for e in range(1, half)]
    base, gram = lower(tiles, cols, factor, first, part, heard, told, rows_grp)
    return sweep(base, gram, factor, sums[0], parts)


def solution(mesh):
    in_specs = (
        P(("grp", "row"), None, None, None, None),
        P(("grp", "row"), None, None),
        P(None, ("grp", "row")),
    )
    out_specs = P(None, ("grp", "row"))
    return jax.shard_map(
        per_device, mesh=mesh, in_specs=in_specs, out_specs=out_specs, check_vma=False
    )
```

```python
import functools

import jax
import jax.numpy as jnp
from jax import lax
from jax.experimental import pallas as pl
from jax.experimental.pallas import tpu as pltpu
from jax.sharding import PartitionSpec as P


floor_value = 1e-06
VMEM = pl.BlockSpec(memory_space=pltpu.VMEM)
SMEM = pl.BlockSpec(memory_space=pltpu.SMEM)
HBM = pl.BlockSpec(memory_space=pltpu.HBM)
f32 = jnp.float32
bf16 = jnp.bfloat16


def call(kernel, in_specs, out_shape, limit, flops, nbytes, scratch=()):
    return pl.pallas_call(
        kernel,
        in_specs=in_specs,
        out_specs=[VMEM] * len(out_shape),
        out_shape=out_shape,
        scratch_shapes=list(scratch),
        compiler_params=pltpu.CompilerParams(vmem_limit_bytes=limit),
        cost_estimate=pl.CostEstimate(flops=flops, bytes_accessed=nbytes, transcendentals=0),
    )


def shape(dims, dtype):
    return jax.ShapeDtypeStruct(dims, dtype)


def dot_nt(a, b):
    return lax.dot_general(a, b, (((1,), (1,)), ((), ())), preferred_element_type=f32)


def position():
    r = lax.axis_index("row")
    return lax.axis_index("grp"), lax.shift_right_logical(r, 1), jnp.bitwise_and(r, 1)


def ahead_kernel(zero_ref):
    zero_ref[...] = jnp.zeros_like(zero_ref)


def ahead(dims):
    return call(ahead_kernel, [], [shape(dims, f32)], 1 << 20, 8 << 30, 24 << 20)()[0]


def mirror_kernel(rows_grp, cols_ref, tiles_ref, factor_ref, zero_ref, keep_ref, send_ref, stage):
    groups = tiles_ref.shape[0]
    half = rows_grp // 2
    slots = min(tiles_ref.shape[1], rows_grp)
    g, _, core = position()
    own = factor_ref[...]
    for h in range(groups):

        @pl.when(h <= g)
        def _():
            for u in range(2 * half):
                stage[u] = zero_ref[...]
            for s in range(slots):
                col = cols_ref[h, s]
                place = col - h * rows_grp
                side = jnp.bitwise_xor(jnp.bitwise_and(place, 1), core)
                unit = side * half + lax.shift_right_arithmetic(place, 1)
                unit = jnp.where(col >= 0, unit, 2 * half)
                stage[unit] = jnp.dot(own, tiles_ref[h, s], preferred_element_type=f32)
            keep_ref[h] = stage[0:half]
            send_ref[h] = stage[half : 2 * half]


def mirror(tiles, cols, factor, zero, rows_grp):
    groups, slots, tile, _ = tiles.shape
    rank = factor.shape[0]
    half = rows_grp // 2
    return call(
        functools.partial(mirror_kernel, rows_grp),
        [SMEM, VMEM, VMEM, VMEM],
        [shape((groups, half, rank, tile), f32)] * 2,
        12 << 20,
        2 * groups * slots * rank * tile * tile,
        groups * slots * tile * tile * 2,
        [pltpu.VMEM((2 * half + 1, rank, tile), f32)],
    )(cols, tiles, factor, zero)


LOWEST = -64
LADDER = (64, 32, 16, 8, 4, 2, 1)


def row_scale(top):
    power = jnp.full(top.shape, 2.0**LOWEST, f32)
    inverse = jnp.full(top.shape, 2.0**-LOWEST, f32)
    steps = jnp.zeros(top.shape, jnp.int32)
    for b in LADDER:
        up = top >= power * 2.0**b
        power = jnp.where(up, power * 2.0**b, power)
        inverse = jnp.where(up, inverse * 2.0**-b, inverse)
        steps = jnp.where(up, steps + b, steps)
    return inverse, steps


def row_power(steps):
    power = jnp.full(steps.shape, 2.0**LOWEST, f32)
    for b in LADDER:
        power = jnp.where(jnp.bitwise_and(steps, b) != 0, power * 2.0**b, power)
    return power


def encode(pay, values):
    rank = values[0].shape[0]
    mid = rank // 2
    top = functools.reduce(jnp.maximum, values)
    inverse, steps = row_scale(jnp.max(top, axis=1, keepdims=True))
    factor = inverse * 2.0**15
    for u, value in enumerate(values):
        q = jnp.minimum((value * factor + 0.5).astype(jnp.int32), 65535)
        word = jnp.bitwise_or(q[:mid], lax.shift_left(q[mid:], 16))
        width = pay.shape[1]
        for j in range(word.shape[1] // width):
            at = (u * word.shape[1] // width + j) * mid
            pay[at : at + mid] = word[:, j * width : (j + 1) * width]
    return steps


def decode(pay, u, power, across=1):
    mid = power.shape[0] // 2
    word = jnp.concatenate([pay[(u + j) * mid : (u + j + 1) * mid] for j in range(across)], axis=1)
    low = jnp.bitwise_and(word, 65535).astype(f32)
    high = jnp.bitwise_and(lax.shift_right_logical(word, 16), 65535).astype(f32)
    return jnp.concatenate([low, high], axis=0) * power


def put_steps(pay, steps):
    rank = steps.shape[0]
    base, wide = pay.shape[0] - 8, pay.shape[1] * 8 // rank
    for i in range(rank // 8):
        pay[base:, i * wide : i * wide + wide] = jnp.broadcast_to(steps[i * 8 : i * 8 + 8], (8, wide))


def get_steps(pay, rank):
    base, wide = pay.shape[0] - 8, pay.shape[1] * 8 // rank
    return jnp.concatenate([pay[base:, i * wide : i * wide + 1] for i in range(rank // 8)], axis=0)


def put_square(pay, base, square):
    rank = square.shape[0]
    rows = rank * rank // pay.shape[1]
    for j in range(rank // rows):
        pay[base : base + rows, j * rank : (j + 1) * rank] = square[j * rows : (j + 1) * rows]


def get_square(pay, base, rank):
    rows = rank * rank // pay.shape[1]
    return jnp.concatenate([pay[base : base + rows, j * rank : (j + 1) * rank] for j in range(rank // rows)], axis=0)


def pack_kernel(groups, half, keep_ref, recv_ref, *refs):
    rows, outs = refs[:half], refs[half:]
    own_ref, mine_ref, gram_ref = outs[:3]
    g, _, _ = position()
    rank = keep_ref.shape[2]
    gram = jnp.zeros((rank, rank), f32)
    for e in range(half):
        mine_ref[e] = rows[e][...]
        gram += dot_nt(rows[e][...], rows[e][...])
    gram_ref[...] = gram
    inverse, steps = row_scale(jnp.max(gram, axis=1, keepdims=True))
    coded = jnp.minimum((gram * (inverse * 2.0**23) + 0.5).astype(jnp.int32), (1 << 24) - 1)
    first = lax.broadcasted_iota(jnp.int32, (rank, rank), 1) == 0
    own_ref[...] = keep_ref[g] + recv_ref[g]
    for d in range(1, groups):
        pay = outs[2 + d]
        t = jnp.bitwise_xor(g, d)
        down = t < g
        sums = [keep_ref[t, u] + recv_ref[t, u] for u in range(half)]
        above = encode(pay, [jnp.where(down, sums[u], rows[u][...].astype(f32)) for u in range(half)])
        exponents = lax.shift_left(jnp.where(first, above, steps), 24)
        put_square(pay, half * rank // 2, jnp.bitwise_or(coded, exponents))


def pack(keep, recv, rows):
    groups, half, rank, tile = keep.shape
    return call(
        functools.partial(pack_kernel, groups, half),
        [VMEM, VMEM] + [VMEM] * half,
        [shape((half, rank, tile), f32), shape((half, rank, tile), bf16), shape((rank, rank), f32)]
        + [shape((half * rank // 2 + rank * rank // tile, tile), jnp.int32)] * (groups - 1),
        16 << 20,
        keep.size * 4,
        keep.size * 8,
    )(keep, recv, *rows)


def split3(value):
    hi = value.astype(bf16)
    rest = value - hi.astype(f32)
    mid = rest.astype(bf16)
    low = (rest - mid.astype(f32)).astype(bf16)
    return hi, mid, low


def merge_kernel(groups, half, own_ref, gram_ref, *refs):
    g, z, _ = position()
    arrived = refs[: groups - 1]
    outs = refs[groups - 1 : groups - 1 + half]
    heard_ref, total_ref, acc = refs[groups - 1 + half :]
    rank = own_ref.shape[1]
    gram = gram_ref[...]
    sums = [own_ref[u] for u in range(half)]
    for d in range(1, groups):
        pay = arrived[d - 1]
        square = get_square(pay, half * rank // 2, rank)
        exponents = lax.shift_right_logical(square, 24)
        gram += jnp.bitwise_and(square, (1 << 24) - 1).astype(f32) * (row_power(exponents[:, 1:2]) * 2.0**-23)
        power = row_power(exponents[:, 0:1]) * 2.0**-15
        above = jnp.bitwise_xor(g, d) > g
        for u in range(half):
            value = decode(pay, u, power)
            sums[u] += jnp.where(above, value, 0.0)
            heard_ref[(d - 1) * half + u] = value.astype(bf16)

    total_ref[...] = gram
    for i, part in enumerate(split3(gram)):
        heard_ref[(groups - 1) * half, :, i * rank : (i + 1) * rank] = part
    for u in range(half):
        acc[u] = sums[u]
    outs[0][...] = acc[z]
    for e in range(1, half):
        put_steps(outs[e], encode(outs[e], [acc[jnp.bitwise_xor(z, e)]]))


def merge(own, gram, arrived):
    half, rank, tile = own.shape
    groups = len(arrived) + 1
    return call(
        functools.partial(merge_kernel, groups, half),
        [VMEM, VMEM] + [VMEM] * (groups - 1),
        [shape((rank, tile), f32)]
        + [shape((rank // 2 * (tile // 128) + 8, 128), jnp.int32)] * (half - 1)
        + [shape(((groups - 1) * half + 1, rank, tile), bf16), shape((rank, rank), f32)],
        16 << 20,
        own.size * 2 * groups,
        own.size * 4 * groups,
        [pltpu.VMEM((half, rank, tile), f32)],
    )(own, gram, *arrived)


def row_products(cols_ref, tiles_ref, held, h, base, rows_grp):
    _, z, core = position()
    half = rows_grp // 2
    total = None
    for s in range(min(tiles_ref.shape[1], rows_grp)):
        col = cols_ref[h, s]
        place = col - h * rows_grp
        side = jnp.bitwise_xor(jnp.bitwise_and(place, 1), core)
        unit = side * half + jnp.bitwise_xor(lax.shift_right_arithmetic(place, 1), z)
        x = held[jnp.where(col >= 0, base + unit, held.shape[0] - 1)]
        term = dot_nt(tiles_ref[h, s], x)
        total = term if total is None else total + term
    return total


def near_kernel(rows_grp, cols_ref, tiles_ref, mine_ref, theirs_ref, out_ref, held):
    g, _, _ = position()
    half = rows_grp // 2
    held[0:half] = mine_ref[...]
    held[half:rows_grp] = theirs_ref[...]
    held[rows_grp] = jnp.zeros_like(held[0])
    out_ref[...] = row_products(cols_ref, tiles_ref, held, g, 0, rows_grp)


def near(tiles, cols, mine, theirs, rows_grp):
    _, slots, tile, _ = tiles.shape
    rank = mine.shape[1]
    return call(
        functools.partial(near_kernel, rows_grp),
        [SMEM, VMEM, VMEM, VMEM],
        [shape((tile, rank), f32)],
        8 << 20,
        2 * slots * rank * tile * tile,
        slots * tile * tile * 2,
        [pltpu.VMEM((rows_grp + 1, rank, tile), bf16)],
    )(cols, tiles, mine, theirs)[0]


def lower_kernel(groups, rows_grp, cols_ref, tiles_ref, factor_ref, near_ref, part_ref, *refs):
    heard_ref, told_ref, out_ref, gram_ref, held, acc, cols, sem = refs
    fetch = pltpu.make_async_copy(cols_ref, cols, sem)
    fetch.start()
    half = rows_grp // 2
    rank = factor_ref.shape[0]
    g, _, _ = position()
    held[groups * rows_grp] = jnp.zeros_like(held[0])
    for d in range(1, groups):
        t = jnp.bitwise_xor(g, d)
        held[pl.ds(t * rows_grp, half)] = heard_ref[(d - 1) * half : d * half]
        held[pl.ds(t * rows_grp + half, half)] = told_ref[(d - 1) * half : d * half]

    gram = part_ref[...]
    for i in range(3):
        gram += told_ref[(groups - 1) * half, :, i * rank : (i + 1) * rank].astype(f32)
    gram_ref[...] = gram
    fitted = lax.dot_general(
        gram,
        factor_ref[...].astype(f32),
        (((0,), (0,)), ((), ())),
        precision=lax.Precision.HIGHEST,
        preferred_element_type=f32,
    )
    acc[...] = near_ref[...]
    fetch.wait()
    for h in range(groups - 1):

        @pl.when(h < g)
        def _():
            acc[...] += row_products(cols, tiles_ref, held, h, h * rows_grp, rows_grp)

    out_ref[...] = acc[...].T - fitted


def lower(tiles, cols, factor, first, part, heard, told, rows_grp):
    groups, slots, tile, _ = tiles.shape
    rank = factor.shape[0]
    return call(
        functools.partial(lower_kernel, groups, rows_grp),
        [HBM] + [VMEM] * 6,
        [shape((rank, tile), f32), shape((rank, rank), f32)],
        20 << 20,
        2 * groups * slots * rank * tile * tile,
        groups * slots * tile * tile * 2,
        [
            pltpu.VMEM((groups * rows_grp + 1, rank, tile), bf16),
            pltpu.VMEM((tile, rank), f32),
            pltpu.SMEM(cols.shape, jnp.int32),
            pltpu.SemaphoreType.DMA(()),
        ],
    )(cols, tiles, factor, first, part, heard, told)


def sweep_kernel(parts, base_ref, gram_ref, factor_ref, own_ref, *refs):
    out_ref = refs[parts]
    rank, tile = factor_ref.shape
    current = factor_ref[...].astype(f32)
    gram = gram_ref[...]
    residual = base_ref[...] + own_ref[...]
    for ref in refs[:parts]:
        residual += decode(ref, 0, row_power(get_steps(ref, rank)) * 2.0**-15, tile // 128)
    eye = lax.broadcasted_iota(jnp.int32, (rank, rank), 0) == lax.broadcasted_iota(jnp.int32, (rank, rank), 1)
    inverse = 1.0 / jnp.sum(jnp.where(eye, gram, 0.0), axis=1, keepdims=True)
    scaled = gram * inverse
    residual = residual * inverse
    least = floor_value - current
    step = 8
    blocks = rank // step
    place = lax.broadcasted_iota(jnp.int32, (step, tile), 0)
    rest = [residual[b * step : (b + 1) * step] for b in range(blocks)]
    for b in range(blocks):
        at = slice(b * step, (b + 1) * step)
        found = rest[b]
        for k in range(step):
            row = b * step + k
            found = jnp.where(place == k, rest[b], found)
            delta = jnp.broadcast_to(jnp.maximum(rest[b], least[at])[k : k + 1], (step, tile))
            for j in range(b, blocks):
                rest[j] = rest[j] - scaled[j * step : (j + 1) * step, row : row + 1] * delta
        out_ref[at] = jnp.maximum(current[at] + found, floor_value)


def sweep(base, gram, factor, own, parts):
    rank, tile = factor.shape
    return call(
        functools.partial(sweep_kernel, len(parts)),
        [VMEM] * (4 + len(parts)),
        [shape((rank, tile), f32)],
        8 << 20,
        2 * rank * rank * tile,
        rank * tile * 4 * (len(parts) + 3),
    )(base, gram, factor, own, *parts)[0]


def per_device(blocks, columns, factor):
    tiles = blocks[0]
    cols = pltpu.with_memory_space_constraint(columns[0], pltpu.HBM)
    rows_grp = lax.axis_size("row")
    groups = lax.axis_size("grp")
    half = rows_grp // 2

    def over_z(x, e):
        return lax.ppermute(x, "row", [(i, ((i // 2) ^ e) * 2 + i % 2) for i in range(rows_grp)])

    def over_core(x):
        return lax.ppermute(x, "row", [(i, i ^ 1) for i in range(rows_grp)])

    def over_grp(x, d):
        return lax.ppermute(x, "grp", [(i, i ^ d) for i in range(groups)])

    zero = ahead(factor.shape)
    rows = [factor]
    for e in range(1, half):
        low = e & -e
        rows.append(over_z(rows[e - low], low))
    keep, send = mirror(tiles, cols, factor, zero, rows_grp)
    recv = over_core(send)
    own, mine, gram, *pays = pack(keep, recv, rows)
    arrived = [over_grp(pay, d + 1) for d, pay in enumerate(pays)]
    theirs = over_core(mine)
    first = near(tiles, cols, mine, theirs, rows_grp)
    *sums, heard, part = merge(own, gram, arrived)
    told = over_core(heard)
    parts = [over_z(sums[e], e) for e in range(1, half)]
    base, gram = lower(tiles, cols, factor, first, part, heard, told, rows_grp)
    return sweep(base, gram, factor, sums[0], parts)


def solution(mesh):
    in_specs = (
        P(("grp", "row"), None, None, None, None),
        P(("grp", "row"), None, None),
        P(None, ("grp", "row")),
    )
    out_specs = P(None, ("grp", "row"))
    return jax.shard_map(
        per_device, mesh=mesh, in_specs=in_specs, out_specs=out_specs, check_vma=False
    )
```
